32 devices in a mesh: fsdp: 8 (over z, y), dp: 4 (over x, core).
Axes of the slice: x: 2, y: 2, z: 4, core: 2. Of those that a mesh axis runs over, the one named last changes fastest.
Arguments:
- tokens: bfloat16 [512, 4096], P('dp', 'fsdp'), may hold values from -6 to 6
- out_grad: bfloat16 [512, 5120], P('dp', 'fsdp'), may hold values from -0.26367188 to 0.26367188
- master: float32 [4096, 5120], P('fsdp'), may hold values from -0.09375 to 0.09375
- moment_one: float32 [4096, 5120], P('fsdp'), may hold values from -3 to 3
- moment_two: float32 [4096, 5120], P('fsdp'), may hold values from 0.1 to 4
- flags: int32 [32, 16], P(('fsdp', 'dp')), may hold values 0 or 1
- steps: int32 [16], replicated, may hold values from 1 to 8
- rate: float32 [1], replicated, may hold values from 0.001 to 0.01
Outputs:
- master_next: float32 [4096, 5120], P('fsdp')
- moment_one_next: float32 [4096, 5120], P('fsdp')
- moment_two_next: float32 [4096, 5120], P('fsdp')
- weight_half: bfloat16 [4096, 5120], P('fsdp')
- steps_next: int32 [16], replicated
- outputs: bfloat16 [512, 5120], P('dp', 'fsdp')
The draws below stay inside these ranges and needn't reach their ends.
All inputs are finite; a program needn't handle non-finite values. No bound on the sum of `flags` on one device may be relied on, other than what follows from the above.
Results may differ from the reference program's by a relative error of at most 0.0049.
Values may be sent and summed in bfloat16 or wider, within the bound.
A program may use at most 128 MiB of HBM per device.

```python
import math
import jax
import jax.numpy as jnp
from jax import lax

D = 4096
R = 5120
BUCKETS = 16
TOK_G = 128
TOKENS = 512
N_FSDP = 8
N_DP = 4


def touch_ends(values, key, smallest, high):
    extent = values.shape
    place = [jax.random.randint(jax.random.fold_in(key, axis), (), 0, extent[axis]) for axis in range(len(extent))]
    values = values.at[tuple(place)].set(smallest)
    longest = extent.index(max(extent))
    place[longest] = (place[longest] + 1) % extent[longest]
    return values.at[tuple(place)].set(high)


def block_scale(rng, extent, cuts, smallest, largest):
    loudness, own = 1.0, jax.random.fold_in(rng, 6)
    for position, shards_of in cuts:
        heights = jnp.exp(jax.random.uniform(jax.random.fold_in(own, position), (shards_of,), jnp.float32, smallest / len(cuts), largest / len(cuts)))
        loudness = loudness * jnp.repeat(heights, extent[position] // shards_of).reshape([-1 if axis == position else 1 for axis in range(len(extent))])
    return loudness


def normal_values(stream_key, dims, spread, limit, cuts=(), kind=jnp.bfloat16):
    values = jax.random.normal(stream_key, dims, jnp.float32) * spread
    if len(cuts) > 0:
        values = block_scale(stream_key, dims, cuts, -0.22, 0.18) * values
    return jnp.clip(values, min=-limit, max=limit).astype(kind)


def setup_inputs(seed: int = 0) -> dict:
    streams_of = jax.random.split(jax.random.key(seed), 9)
    return {
        "tokens": normal_values(streams_of[0], (TOKENS, D), 1.0, 6.0, ((0, 4), (1, 8))),
        "out_grad": normal_values(streams_of[1], (TOKENS, R), (1.0 / (TOK_G * N_DP) ** 0.5), 0.26367188, ((0, 4), (1, 8))),
        "master": normal_values(streams_of[2], (D, R), D ** -0.5, 0.09375, ((0, 8),), jnp.float32),
        "moment_one": normal_values(streams_of[3], (D, R), 0.5, 3.0, ((0, 8),), jnp.float32),
        "moment_two": jnp.clip(jnp.exp(math.log(4.0) - 3.6888794 * jax.random.uniform(streams_of[4], (D, R), jnp.float32) ** block_scale(streams_of[4], (D, R), ((0, 8),), -0.2, 0.2)), 0.1, 4.0),
        "flags": touch_ends((jax.random.randint(streams_of[5], (N_FSDP * N_DP, BUCKETS), 0, N_FSDP * N_DP * 3 // 2) < 1).astype(jnp.int32), jax.random.fold_in(streams_of[5], 1), 0, 1),
        "steps": touch_ends(jax.random.randint(streams_of[6], (BUCKETS,), 1, 9), jax.random.fold_in(streams_of[6], 1), 1, 8).astype(jnp.int32),
        "rate": jnp.clip(jnp.exp(jax.random.uniform(streams_of[7], (1,), jnp.float32, math.log(0.001), math.log(0.01))), 0.001, 0.01),
    }


first_decay = 0.9
second_decay = 0.95
epsilon = 1e-08

def reference(tokens, out_grad, master, moment_one, moment_two, flags, steps, rate):
    gradient = lax.dot_general(tokens, out_grad, (((0,), (0,)), ((), ())), preferred_element_type=jnp.float32)
    bucket_width = master.shape[1] // BUCKETS
    counts = lax.optimization_barrier(jnp.sum(flags, axis=0)).astype(jnp.int32)
    commit_bucket = counts == 0
    commit = jnp.repeat(commit_bucket, bucket_width)[None, :]
    times = jnp.repeat(steps + 1, bucket_width).astype(jnp.float32)[None, :]
    first = first_decay * moment_one + (1.0 - first_decay) * gradient
    second = second_decay * moment_two + (1.0 - second_decay) * gradient * gradient
    fix_one = 1.0 - jnp.power(jnp.float32(first_decay), times)
    fix_two = 1.0 - jnp.power(jnp.float32(second_decay), times)
    candidate = master - rate[0] * (first / fix_one) / (jnp.sqrt(second / fix_two) + epsilon)
    master_next = jnp.where(commit, candidate, master)
    moment_one_next = jnp.where(commit, first, moment_one)
    moment_two_next = jnp.where(commit, second, moment_two)
    weight_half = master_next.astype(jnp.bfloat16)
    steps_next = steps + commit_bucket.astype(jnp.int32)
    outputs = jnp.dot(tokens, weight_half, preferred_element_type=jnp.float32).astype(jnp.bfloat16)
    return (master_next, moment_one_next, moment_two_next, weight_half, steps_next, outputs)
```

```python
import jax
import jax.numpy as jnp
from jax import lax
from jax.sharding import PartitionSpec as P

BUCKETS = 16


first_decay = 0.9
second_decay = 0.95
epsilon = 1e-08


def local(tokens, out_grad, master, moment_one, moment_two, flags, steps, rate):
    width_out = master.shape[1]
    bucket_width = width_out // BUCKETS
    contract_rows = (((0,), (0,)), ((), ()))
    rows = lax.all_gather(tokens, "dp", axis=0, tiled=True)
    grads = lax.all_gather(
        lax.all_gather(out_grad, "fsdp", axis=1, tiled=True), "dp", axis=0, tiled=True
    )
    counts = lax.psum(flags[0], ("fsdp", "dp"))
    gradient = lax.dot_general(
        rows, grads, contract_rows, preferred_element_type=jnp.float32
    )
    commit_bucket = counts == 0
    commit = jnp.repeat(commit_bucket, bucket_width)[None, :]
    times = jnp.repeat(steps + 1, bucket_width).astype(jnp.float32)[None, :]
    first = first_decay * moment_one + (1.0 - first_decay) * gradient
    second = second_decay * moment_two + (1.0 - second_decay) * gradient * gradient
    fix_one = 1.0 - jnp.power(jnp.float32(first_decay), times)
    fix_two = 1.0 - jnp.power(jnp.float32(second_decay), times)
    candidate = master - rate[0] * (first / fix_one) / (jnp.sqrt(second / fix_two) + epsilon)
    master_next = jnp.where(commit, candidate, master)
    moment_one_next = jnp.where(commit, first, moment_one)
    moment_two_next = jnp.where(commit, second, moment_two)
    weight_half = master_next.astype(jnp.bfloat16)
    steps_next = steps + commit_bucket.astype(jnp.int32)
    share = lax.dot_general(
        tokens, weight_half, (((1,), (0,)), ((), ())), preferred_element_type=jnp.float32
    ).astype(jnp.bfloat16)
    shards = lax.axis_size("fsdp")
    pieces = share.reshape(share.shape[0], shards, -1).transpose(1, 0, 2)
    result = jnp.sum(
        lax.all_to_all(pieces, "fsdp", 0, 0).astype(jnp.float32), axis=0
    )
    return (
        master_next,
        moment_one_next,
        moment_two_next,
        weight_half,
        steps_next,
        result.astype(jnp.bfloat16),
    )


def solution(mesh):
    in_specs = (
        P("dp", "fsdp"),
        P("dp", "fsdp"),
        P("fsdp", None),
        P("fsdp", None),
        P("fsdp", None),
        P(("fsdp", "dp"), None),
        P(),
        P(),
    )
    out_specs = (
        P("fsdp", None),
        P("fsdp", None),
        P("fsdp", None),
        P("fsdp", None),
        P(),
        P("dp", "fsdp"),
    )
    return jax.shard_map(local, mesh=mesh, in_specs=in_specs, out_specs=out_specs, check_vma=False)
```

```python
import functools

import jax
import jax.numpy as jnp
from jax import lax
from jax.experimental import pallas as pl
from jax.experimental.pallas import tpu as pltpu
from jax.sharding import PartitionSpec as P

BUCKETS = 16


first_decay = 0.9
second_decay = 0.95
epsilon = 1e-08


def plain(tokens, out_grad, master, moment_one, moment_two, flags, steps, rate):
    width_out = master.shape[1]
    bucket_width = width_out // BUCKETS
    contract_rows = (((0,), (0,)), ((), ()))
    rows = lax.all_gather(tokens, "dp", axis=0, tiled=True)
    grads = lax.all_gather(
        lax.all_gather(out_grad, "fsdp", axis=1, tiled=True), "dp", axis=0, tiled=True
    )
    counts = lax.psum(flags[0], ("fsdp", "dp"))
    gradient = lax.dot_general(
        rows, grads, contract_rows, preferred_element_type=jnp.float32
    )
    commit_bucket = counts == 0
    commit = jnp.repeat(commit_bucket, bucket_width)[None, :]
    times = jnp.repeat(steps + 1, bucket_width).astype(jnp.float32)[None, :]
    first = first_decay * moment_one + (1.0 - first_decay) * gradient
    second = second_decay * moment_two + (1.0 - second_decay) * gradient * gradient
    fix_one = 1.0 - jnp.power(jnp.float32(first_decay), times)
    fix_two = 1.0 - jnp.power(jnp.float32(second_decay), times)
    candidate = master - rate[0] * (first / fix_one) / (jnp.sqrt(second / fix_two) + epsilon)
    master_next = jnp.where(commit, candidate, master)
    moment_one_next = jnp.where(commit, first, moment_one)
    moment_two_next = jnp.where(commit, second, moment_two)
    weight_half = master_next.astype(jnp.bfloat16)
    steps_next = steps + commit_bucket.astype(jnp.int32)
    share = lax.dot_general(
        tokens, weight_half, (((1,), (0,)), ((), ())), preferred_element_type=jnp.float32
    ).astype(jnp.bfloat16)
    shards = lax.axis_size("fsdp")
    pieces = share.reshape(share.shape[0], shards, -1).transpose(1, 0, 2)
    result = jnp.sum(
        lax.all_to_all(pieces, "fsdp", 0, 0).astype(jnp.float32), axis=0
    )
    return (
        master_next,
        moment_one_next,
        moment_two_next,
        weight_half,
        steps_next,
        result.astype(jnp.bfloat16),
    )


def exchange(
    nf, bucket_width,
    tok, tokt, og, flag, coef, master, one, two,
    master_o, one_o, two_o, half_o, count_o, out_o,
    obuf, tbuf, grad, commit, fl, ysend, yrecv, zsend, zrecv, acc,
    read_sem, loc_sem,
    fz_s, fz_r, f_s, f_r, t_s, t_r,
    z_s, z_r, y_s, y_r, x_s, x_r, c_s, c_r, d_s, d_r, ry_s, ry_r, rz_s, rz_r,
):
    nz = nf // 2
    f, d = lax.axis_index("fsdp"), lax.axis_index("dp")
    yp = f + 1 - 2 * lax.rem(f, 2)
    sib, xn = d + 1 - 2 * lax.rem(d, 2), lax.rem(d + 2, 4)
    toks, width = og.shape
    rows = tok.shape[1]

    def peer(k):
        return lax.rem(f + 2 * k, nf)

    def column(par, k):
        return lax.rem(f + par * (1 - 2 * lax.rem(f, 2)) + 2 * k, nf)

    def span(block):
        return pl.ds(pl.multiple_of(block * width, 128), width)

    def slot(dd):
        return pl.ds(pl.multiple_of(dd * toks, 128), toks)

    def piece(block, dd):
        return obuf.at[block, slot(dd)]

    def send(src, dst, ssem, rsem, ff, dd):
        return pltpu.make_async_remote_copy(
            src_ref=src, dst_ref=dst, send_sem=ssem, recv_sem=rsem,
            device_id={"fsdp": ff, "dp": dd}, device_id_type=pl.DeviceIdType.MESH,
        )

    def z_copy(k):
        return send(og, piece(f, d), z_s.at[k], z_r.at[nz - k], peer(k), d)

    def y_copy(k):
        p = piece(column(0, k), d)
        return send(p, p, y_s.at[k], y_r.at[k], yp, d)

    def x_copy(par, k):
        p, j = piece(column(par, k), d), par * nz + k
        return send(p, p, x_s.at[j], x_r.at[j], f, xn)

    def c_copy(par, k):
        p, j = piece(column(par, k), d), par * nz + k
        return send(p, p, c_s.at[j], c_r.at[j], f, sib)

    def d_copy(par, k):
        p, j = piece(column(par, k), xn), par * nz + k
        return send(p, p, d_s.at[j], d_r.at[j], f, sib)

    def t_copy(i):
        p = tbuf.at[:, slot(xn if i == 2 else d)]
        return send(p if i == 2 else tokt, p, t_s.at[i], t_r.at[i], f, xn if i == 0 else sib)

    def fz_copy(k):
        return send(flag, fl.at[nz - k], fz_s.at[k], fz_r.at[nz - k], peer(k), d)

    def f_copy(i):
        n = nz << i
        ff, dd = ((yp, d), (f, xn), (f, sib))[i]
        return send(fl.at[pl.ds(0, n)], fl.at[pl.ds(n, n)], f_s.at[i], f_r.at[i], ff, dd)

    def ry_copy(k):
        return send(ysend.at[k], yrecv.at[k], ry_s.at[k], ry_r.at[k], yp, d)

    def rz_copy(k):
        return send(zsend.at[k], zrecv.at[nz - k], rz_s.at[k], rz_r.at[nz - k], peer(k), d)

    state = ((master, master_o), (one, one_o), (two, two_o))

    def read(i, par, k):
        cols = span(column(par, k))
        return pltpu.make_async_copy(
            state[i][0].at[:, cols], state[i][1].at[:, cols], read_sem.at[i, par * nz + k]
        )

    @pl.loop(0, nz)
    def _(k):
        for par in (1, 0):
            for i in range(3):
                read(i, par, k).start()

    own = (
        pltpu.make_async_copy(og, piece(f, d), loc_sem.at[0]),
        pltpu.make_async_copy(tokt, tbuf.at[:, slot(d)], loc_sem.at[1]),
        pltpu.make_async_copy(flag, fl.at[0], loc_sem.at[2]),
    )
    for copy in own:
        copy.start()

    barrier = pltpu.get_barrier_semaphore()
    near = [(peer(k), d) for k in range(1, nz)] + [(yp, d), (f, xn), (f, sib)]
    for ff, dd in near:
        pl.semaphore_signal(
            barrier, inc=1, device_id={"fsdp": ff, "dp": dd},
            device_id_type=pl.DeviceIdType.MESH,
        )
    pl.semaphore_wait(barrier, len(near))

    for k in range(1, nz):
        fz_copy(k).start()
    t_copy(0).start()
    t_copy(1).start()
    for k in range(1, nz):
        z_copy(k).start()
    for copy in own:
        copy.wait()
    y_copy(0).start()
    x_copy(0, 0).start()
    c_copy(0, 0).start()
    for k in range(1, nz):
        fz_copy(k).wait_send()
        fz_copy(nz - k).wait_recv()
    f_copy(0).start()
    y_copy(0).wait_recv()
    x_copy(1, 0).start()
    c_copy(1, 0).start()
    f_copy(0).wait()
    f_copy(1).start()
    t_copy(0).wait()
    t_copy(2).start()
    f_copy(1).wait()
    f_copy(2).start()
    t_copy(1).wait()
    t_copy(2).wait()
    f_copy(2).wait()

    counts = jnp.sum(fl[...], axis=0)
    count_o[...] = counts
    buckets = commit.shape[1] // bucket_width
    where = lax.broadcasted_iota(jnp.int32, commit.shape, 1) // bucket_width
    ok = jnp.zeros(commit.shape, jnp.int32)
    for b in range(buckets):
        ok = jnp.where(where == b, counts[:, b : b + 1], ok)
    commit[...] = ok

    @pl.loop(0, 2 * nz)
    def _(step):
        k = step // 2
        par = 1 - lax.rem(step, 2)

        @pl.when((par == 1) & (k + 1 < nz))
        def _():
            n = k + 1
            send(og, piece(f, d), z_s.at[n], z_r.at[n], peer(n), d).wait_recv()
            y_copy(n).start()
            y_copy(n).wait_recv()
            for q in (1, 0):
                x_copy(q, n).start()
                c_copy(q, n).start()

        x_copy(par, k).wait_recv()
        d_copy(par, k).start()
        c_copy(par, k).wait_recv()
        d_copy(par, k).wait_recv()
        for i in range(3):
            read(i, par, k).wait()
        block = column(par, k)
        cols = span(block)
        grad[...] = jnp.dot(tbuf[...], obuf[block], preferred_element_type=jnp.float32)
        scale_one = coef[0:1, cols]
        scale_two = coef[1:2, cols]
        keep = commit[0:1, cols] == 0

        @pl.loop(0, rows // 16)
        def _(r):
            lines = pl.ds(pl.multiple_of(r * 16, 16), 16)
            g = grad[lines, :]
            old = master_o[lines, cols]
            old_one = one_o[lines, cols]
            old_two = two_o[lines, cols]
            first = first_decay * old_one + (1.0 - first_decay) * g
            second = second_decay * old_two + (1.0 - second_decay) * g * g
            new = old - (first * scale_one) / (jnp.sqrt(second * scale_two) + epsilon)
            new = jnp.where(keep, new, old)
            master_o[lines, cols] = new
            half_o[lines, cols] = new.astype(jnp.bfloat16)
            one_o[lines, cols] = jnp.where(keep, first, old_one)
            two_o[lines, cols] = jnp.where(keep, second, old_two)

        share = jnp.dot(tok[...], half_o[:, cols], preferred_element_type=jnp.float32)

        @pl.when(par == 1)
        def _():
            ysend[k] = share.astype(jnp.bfloat16)
            ry_copy(k).start()

        @pl.when(par == 0)
        def _():
            ry_copy(k).wait_recv()
            both = share + yrecv[k].astype(jnp.float32)

            @pl.when(k == 0)
            def _():
                acc[...] = both

            @pl.when(k > 0)
            def _():
                zsend[k] = both.astype(jnp.bfloat16)
                rz_copy(k).start()

    total = acc[...]
    for k in range(1, nz):
        rz_copy(nz - k).wait_recv()
        total = total + zrecv[k].astype(jnp.float32)
    out_o[...] = total.astype(jnp.bfloat16)

    for k in range(nz):
        y_copy(k).wait_send()
        ry_copy(k).wait_send()
        if k > 0:
            z_copy(k).wait_send()
            rz_copy(k).wait_send()
        for par in (0, 1):
            x_copy(par, k).wait_send()
            c_copy(par, k).wait_send()
            d_copy(par, k).wait_send()


def local(tokens, out_grad, master, moment_one, moment_two, flags, steps, rate):
    nf, nd = lax.axis_size("fsdp"), lax.axis_size("dp")
    toks, width = out_grad.shape
    rows, columns = master.shape
    nz = nf // 2
    if width % 128 or toks % 128 or rows % 128 or nd != 4 or nf % 2 or nf < 4:
        return plain(
            tokens, out_grad, master, moment_one, moment_two, flags, steps, rate
        )
    bucket_width = columns // BUCKETS
    times = (steps + 1).astype(jnp.float32)
    one = rate[0] / (1.0 - jnp.power(jnp.float32(first_decay), times))
    two = 1.0 / (1.0 - jnp.power(jnp.float32(second_decay), times))
    coef = jnp.repeat(jnp.stack([one, two]), bucket_width, axis=1)
    flag = jnp.pad(flags, ((0, 7), (0, 128 - BUCKETS)))
    vmem = pl.BlockSpec(memory_space=pltpu.VMEM)
    anyw = pl.BlockSpec(memory_space=pl.ANY)
    full = (rows, columns)
    bf, f32, dma = jnp.bfloat16, jnp.float32, pltpu.SemaphoreType.DMA
    pairs = lambda n: [dma((n,)), dma((n,))]
    master_n, one_n, two_n, half, counts, outputs = pl.pallas_call(
        functools.partial(exchange, nf, bucket_width),
        out_shape=(
            pltpu.VMEM(full, f32),
            pltpu.VMEM(full, f32),
            pltpu.VMEM(full, f32),
            jax.ShapeDtypeStruct(full, bf),
            jax.ShapeDtypeStruct((8, 128), jnp.int32),
            jax.ShapeDtypeStruct((toks, width), bf),
        ),
        in_specs=[vmem] * 5 + [anyw] * 3,
        out_specs=[vmem] * 6,
        scratch_shapes=[
            pltpu.VMEM((nf, nd * toks, width), bf),
            pltpu.VMEM((rows, nd * toks), bf),
            pltpu.VMEM((rows, width), f32),
            pltpu.VMEM((8, columns), jnp.int32),
            pltpu.VMEM((8 * nz, 8, 128), jnp.int32),
            pltpu.VMEM((nz, toks, width), bf),
            pltpu.VMEM((nz, toks, width), bf),
            pltpu.VMEM((nz, toks, width), bf),
            pltpu.VMEM((nz, toks, width), bf),
            pltpu.VMEM((toks, width), f32),
            dma((3, nf)),
            dma((3,)),
        ]
        + pairs(nz) + pairs(3) + pairs(3)
        + pairs(nz) + pairs(nz) + pairs(nf) + pairs(nf) + pairs(nf) + pairs(nz) + pairs(nz),
        compiler_params=pltpu.CompilerParams(
            collective_id=0, has_side_effects=True, vmem_limit_bytes=24000000
        ),
    )(tokens, tokens.T, out_grad, flag, coef, master, moment_one, moment_two)
    steps_next = steps + (counts[0, :BUCKETS] == 0).astype(jnp.int32)
    return master_n, one_n, two_n, half, steps_next, outputs


def solution(mesh):
    in_specs = (
        P("dp", "fsdp"),
        P("dp", "fsdp"),
        P("fsdp", None),
        P("fsdp", None),
        P("fsdp", None),
        P(("fsdp", "dp"), None),
        P(),
        P(),
    )
    out_specs = (
        P("fsdp", None),
        P("fsdp", None),
        P("fsdp", None),
        P("fsdp", None),
        P(),
        P("dp", "fsdp"),
    )
    return jax.shard_map(local, mesh=mesh, in_specs=in_specs, out_specs=out_specs, check_vma=False)
```

```python
import functools

import jax
import jax.numpy as jnp
from jax import lax
from jax.experimental import pallas as pl
from jax.experimental.pallas import tpu as pltpu
from jax.sharding import PartitionSpec as P

BUCKETS = 16


first_decay = 0.9
second_decay = 0.95
epsilon = 1e-08


def plain(tokens, out_grad, master, moment_one, moment_two, flags, steps, rate):
    width_out = master.shape[1]
    bucket_width = width_out // BUCKETS
    contract_rows = (((0,), (0,)), ((), ()))
    rows = lax.all_gather(tokens, "dp", axis=0, tiled=True)
    grads = lax.all_gather(
        lax.all_gather(out_grad, "fsdp", axis=1, tiled=True), "dp", axis=0, tiled=True
    )
    counts = lax.psum(flags[0], ("fsdp", "dp"))
    gradient = lax.dot_general(
        rows, grads, contract_rows, preferred_element_type=jnp.float32
    )
    commit_bucket = counts == 0
    commit = jnp.repeat(commit_bucket, bucket_width)[None, :]
    times = jnp.repeat(steps + 1, bucket_width).astype(jnp.float32)[None, :]
    first = first_decay * moment_one + (1.0 - first_decay) * gradient
    second = second_decay * moment_two + (1.0 - second_decay) * gradient * gradient
    fix_one = 1.0 - jnp.power(jnp.float32(first_decay), times)
    fix_two = 1.0 - jnp.power(jnp.float32(second_decay), times)
    candidate = master - rate[0] * (first / fix_one) / (jnp.sqrt(second / fix_two) + epsilon)
    master_next = jnp.where(commit, candidate, master)
    moment_one_next = jnp.where(commit, first, moment_one)
    moment_two_next = jnp.where(commit, second, moment_two)
    weight_half = master_next.astype(jnp.bfloat16)
    steps_next = steps + commit_bucket.astype(jnp.int32)
    share = lax.dot_general(
        tokens, weight_half, (((1,), (0,)), ((), ())), preferred_element_type=jnp.float32
    ).astype(jnp.bfloat16)
    shards = lax.axis_size("fsdp")
    pieces = share.reshape(share.shape[0], shards, -1).transpose(1, 0, 2)
    result = jnp.sum(
        lax.all_to_all(pieces, "fsdp", 0, 0).astype(jnp.float32), axis=0
    )
    return (
        master_next,
        moment_one_next,
        moment_two_next,
        weight_half,
        steps_next,
        result.astype(jnp.bfloat16),
    )


def exchange(
    nf, bucket_width,
    tok, tokt, og, flag, coef, master, one, two,
    master_o, one_o, two_o, half_o, count_o, out_o,
    obuf, tbuf, grad, commit, fl, ysend, yrecv, zsend, zrecv, acc,
    read_sem, loc_sem,
    fz_s, fz_r, f_s, f_r, t_s, t_r,
    z_s, z_r, y_s, y_r, x_s, x_r, c_s, c_r, d_s, d_r, ry_s, ry_r, rz_s, rz_r,
):
    nz = nf // 2
    f, d = lax.axis_index("fsdp"), lax.axis_index("dp")
    yp = f + 1 - 2 * lax.rem(f, 2)
    sib, xn = d + 1 - 2 * lax.rem(d, 2), lax.rem(d + 2, 4)
    toks, width = og.shape
    rows = tok.shape[1]

    def peer(k):
        return lax.rem(f + 2 * k, nf)

    def column(par, k):
        return lax.rem(f + par * (1 - 2 * lax.rem(f, 2)) + 2 * k, nf)

    def span(block):
        return pl.ds(pl.multiple_of(block * width, 128), width)

    def slot(dd):
        return pl.ds(pl.multiple_of(dd * toks, 128), toks)

    def piece(block, dd):
        return obuf.at[block, slot(dd)]

    def send(src, dst, ssem, rsem, ff, dd):
        return pltpu.make_async_remote_copy(
            src_ref=src, dst_ref=dst, send_sem=ssem, recv_sem=rsem,
            device_id={"fsdp": ff, "dp": dd}, device_id_type=pl.DeviceIdType.MESH,
        )

    def z_copy(k):
        return send(og, piece(f, d), z_s.at[k], z_r.at[nz - k], peer(k), d)

    def y_copy(k):
        p = piece(column(0, k), d)
        return send(p, p, y_s.at[k], y_r.at[k], yp, d)

    def x_copy(par, k):
        p, j = piece(column(par, k), d), par * nz + k
        return send(p, p, x_s.at[j], x_r.at[j], f, xn)

    def c_copy(par, k):
        p, j = piece(column(par, k), d), par * nz + k
        return send(p, p, c_s.at[j], c_r.at[j], f, sib)

    def d_copy(par, k):
        p, j = piece(column(par, k), xn), par * nz + k
        return send(p, p, d_s.at[j], d_r.at[j], f, sib)

    def t_copy(i):
        p = tbuf.at[:, slot(xn if i == 2 else d)]
        return send(p if i == 2 else tokt, p, t_s.at[i], t_r.at[i], f, xn if i == 0 else sib)

    def fz_copy(k):
        return send(flag, fl.at[nz - k], fz_s.at[k], fz_r.at[nz - k], peer(k), d)

    def f_copy(i):
        n = nz << i
        ff, dd = ((yp, d), (f, xn), (f, sib))[i]
        return send(fl.at[pl.ds(0, n)], fl.at[pl.ds(n, n)], f_s.at[i], f_r.at[i], ff, dd)

    def ry_copy(k):
        return send(ysend.at[k], yrecv.at[k], ry_s.at[k], ry_r.at[k], yp, d)

    def rz_copy(k):
        return send(zsend.at[k], zrecv.at[nz - k], rz_s.at[k], rz_r.at[nz - k], peer(k), d)

    state = ((master, master_o), (one, one_o), (two, two_o))

    def read(i, par, k):
        cols = span(column(par, k))
        return pltpu.make_async_copy(
            state[i][0].at[:, cols], state[i][1].at[:, cols], read_sem.at[i, par * nz + k]
        )

    @pl.loop(0, nz)
    def _(k):
        for par in (1, 0):
            for i in range(3):
                read(i, par, k).start()

    own = (
        pltpu.make_async_copy(og, piece(f, d), loc_sem.at[0]),
        pltpu.make_async_copy(tokt, tbuf.at[:, slot(d)], loc_sem.at[1]),
        pltpu.make_async_copy(flag, fl.at[0], loc_sem.at[2]),
    )
    for copy in own:
        copy.start()

    barrier = pltpu.get_barrier_semaphore()
    near = [(peer(k), d) for k in range(1, nz)] + [(yp, d), (f, xn), (f, sib)]
    for ff, dd in near:
        pl.semaphore_signal(
            barrier, inc=1, device_id={"fsdp": ff, "dp": dd},
            device_id_type=pl.DeviceIdType.MESH,
        )
    pl.semaphore_wait(barrier, len(near))

    for k in range(1, nz):
        fz_copy(k).start()
    t_copy(0).start()
    t_copy(1).start()
    for k in range(1, nz):
        z_copy(k).start()
    for copy in own:
        copy.wait()
    y_copy(0).start()
    x_copy(0, 0).start()
    c_copy(0, 0).start()
    for k in range(1, nz):
        fz_copy(k).wait_send()
        fz_copy(nz - k).wait_recv()
    f_copy(0).start()
    y_copy(0).wait_recv()
    x_copy(1, 0).start()
    c_copy(1, 0).start()
    f_copy(0).wait()
    f_copy(1).start()
    t_copy(0).wait()
    t_copy(2).start()
    f_copy(1).wait()
    f_copy(2).start()
    t_copy(1).wait()
    t_copy(2).wait()
    f_copy(2).wait()

    counts = jnp.sum(fl[...], axis=0)
    count_o[...] = counts
    buckets = commit.shape[1] // bucket_width
    where = lax.broadcasted_iota(jnp.int32, commit.shape, 1) // bucket_width
    ok = jnp.zeros(commit.shape, jnp.int32)
    for b in range(buckets):
        ok = jnp.where(where == b, counts[:, b : b + 1], ok)
    commit[...] = ok

    @pl.loop(0, 2 * nz)
    def _(step):
        k = step // 2
        par = 1 - lax.rem(step, 2)

        @pl.when((par == 1) & (k + 1 < nz))
        def _():
            n = k + 1
            send(og, piece(f, d), z_s.at[n], z_r.at[n], peer(n), d).wait_recv()
            y_copy(n).start()
            y_copy(n).wait_recv()
            for q in (1, 0):
                x_copy(q, n).start()
                c_copy(q, n).start()

        x_copy(par, k).wait_recv()
        d_copy(par, k).start()
        c_copy(par, k).wait_recv()
        d_copy(par, k).wait_recv()
        for i in range(3):
            read(i, par, k).wait()
        block = column(par, k)
        cols = span(block)
        grad[...] = jnp.dot(tbuf[...], obuf[block], preferred_element_type=jnp.float32)
        scale_one = coef[0:1, cols]
        scale_two = coef[1:2, cols]
        keep = commit[0:1, cols] == 0

        @pl.loop(0, rows // 64, unroll=1)
        def _(r):
            lines = pl.ds(pl.multiple_of(r * 64, 64), 64)
            g = grad[lines, :]
            old = master_o[lines, cols]
            old_one = one_o[lines, cols]
            old_two = two_o[lines, cols]
            first = first_decay * old_one + (1.0 - first_decay) * g
            second = second_decay * old_two + (1.0 - second_decay) * g * g
            fixed = second * scale_two
            new = old - (first * scale_one) / (fixed * lax.rsqrt(fixed) + epsilon)
            new = jnp.where(keep, new, old)
            master_o[lines, cols] = new
            half_o[lines, cols] = new.astype(jnp.bfloat16)
            one_o[lines, cols] = jnp.where(keep, first, old_one)
            two_o[lines, cols] = jnp.where(keep, second, old_two)

        share = jnp.dot(tok[...], half_o[:, cols], preferred_element_type=jnp.float32)

        @pl.when(par == 1)
        def _():
            ysend[k] = share.astype(jnp.bfloat16)
            ry_copy(k).start()

        @pl.when(par == 0)
        def _():
            ry_copy(k).wait_recv()
            both = share + yrecv[k].astype(jnp.float32)

            @pl.when(k == 0)
            def _():
                acc[...] = both

            @pl.when(k > 0)
            def _():
                zsend[k] = both.astype(jnp.bfloat16)
                rz_copy(k).start()

    total = acc[...]
    for k in range(1, nz):
        rz_copy(nz - k).wait_recv()
        total = total + zrecv[k].astype(jnp.float32)
    out_o[...] = total.astype(jnp.bfloat16)

    for k in range(nz):
        y_copy(k).wait_send()
        ry_copy(k).wait_send()
        if k > 0:
            z_copy(k).wait_send()
            rz_copy(k).wait_send()
        for par in (0, 1):
            x_copy(par, k).wait_send()
            c_copy(par, k).wait_send()
            d_copy(par, k).wait_send()


def local(tokens, out_grad, master, moment_one, moment_two, flags, steps, rate):
    nf, nd = lax.axis_size("fsdp"), lax.axis_size("dp")
    toks, width = out_grad.shape
    rows, columns = master.shape
    nz = nf // 2
    if width % 128 or toks % 128 or rows % 128 or nd != 4 or nf % 2 or nf < 4:
        return plain(
            tokens, out_grad, master, moment_one, moment_two, flags, steps, rate
        )
    bucket_width = columns // BUCKETS
    times = (steps + 1).astype(jnp.float32)
    one = rate[0] / (1.0 - jnp.power(jnp.float32(first_decay), times))
    two = 1.0 / (1.0 - jnp.power(jnp.float32(second_decay), times))
    coef = jnp.repeat(jnp.stack([one, two]), bucket_width, axis=1)
    flag = jnp.pad(flags, ((0, 7), (0, 128 - BUCKETS)))
    vmem = pl.BlockSpec(memory_space=pltpu.VMEM)
    anyw = pl.BlockSpec(memory_space=pl.ANY)
    full = (rows, columns)
    bf, f32, dma = jnp.bfloat16, jnp.float32, pltpu.SemaphoreType.DMA
    pairs = lambda n: [dma((n,)), dma((n,))]
    master_n, one_n, two_n, half, counts, outputs = pl.pallas_call(
        functools.partial(exchange, nf, bucket_width),
        out_shape=(
            pltpu.VMEM(full, f32),
            pltpu.VMEM(full, f32),
            pltpu.VMEM(full, f32),
            jax.ShapeDtypeStruct(full, bf),
            jax.ShapeDtypeStruct((8, 128), jnp.int32),
            jax.ShapeDtypeStruct((toks, width), bf),
        ),
        in_specs=[vmem] * 5 + [anyw] * 3,
        out_specs=[vmem] * 6,
        scratch_shapes=[
            pltpu.VMEM((nf, nd * toks, width), bf),
            pltpu.VMEM((rows, nd * toks), bf),
            pltpu.VMEM((rows, width), f32),
            pltpu.VMEM((8, columns), jnp.int32),
            pltpu.VMEM((8 * nz, 8, 128), jnp.int32),
            pltpu.VMEM((nz, toks, width), bf),
            pltpu.VMEM((nz, toks, width), bf),
            pltpu.VMEM((nz, toks, width), bf),
            pltpu.VMEM((nz, toks, width), bf),
            pltpu.VMEM((toks, width), f32),
            dma((3, nf)),
            dma((3,)),
        ]
        + pairs(nz) + pairs(3) + pairs(3)
        + pairs(nz) + pairs(nz) + pairs(nf) + pairs(nf) + pairs(nf) + pairs(nz) + pairs(nz),
        compiler_params=pltpu.CompilerParams(
            collective_id=0, has_side_effects=True, vmem_limit_bytes=24000000
        ),
    )(tokens, tokens.T, out_grad, flag, coef, master, moment_one, moment_two)
    steps_next = steps + (counts[0, :BUCKETS] == 0).astype(jnp.int32)
    return master_n, one_n, two_n, half, steps_next, outputs


def solution(mesh):
    in_specs = (
        P("dp", "fsdp"),
        P("dp", "fsdp"),
        P("fsdp", None),
        P("fsdp", None),
        P("fsdp", None),
        P(("fsdp", "dp"), None),
        P(),
        P(),
    )
    out_specs = (
        P("fsdp", None),
        P("fsdp", None),
        P("fsdp", None),
        P("fsdp", None),
        P(),
        P("dp", "fsdp"),
    )
    return jax.shard_map(local, mesh=mesh, in_specs=in_specs, out_specs=out_specs, check_vma=False)
```
